256 devices in a mesh: dp: 4 (over y), ctx: 64 (over x, z, core).
Axes of the slice: x: 4, y: 4, z: 8, core: 2. Of those that a mesh axis runs over, the one named last changes fastest.
Arguments:
- tokens: bfloat16 [4, 24576, 1024], P('dp', 'ctx'), may hold values from -6 to 6
- modality: int32 [4, 24576], P('dp', 'ctx'), may hold values 0 or 1
- type_embed: bfloat16 [2, 1024], replicated, may hold values from -6 to 6
- dest_shard: int32 [4, 24576], P('dp'), may hold values from 0 to 63, as said below
- dest_row: int32 [4, 24576], P('dp'), may hold values from 0 to 383, as said below
- segments: int32 [4, 24576], P('dp'), may hold values from 0 to 127, never falling along the last dimension, each value on 1 to 384 neighbouring positions
- w_qkv: bfloat16 [1024, 3072], P('ctx', 'dp')
- w_out: bfloat16 [1024, 1024], P('ctx', 'dp'), may hold values from -0.1875 to 0.1875
- w_up: bfloat16 [1024, 2048], P('ctx', 'dp'), may hold values from -0.1875 to 0.1875
- w_down: bfloat16 [2048, 1024], P('ctx', 'dp'), may hold values from -0.125 to 0.125
Outputs:
- encoded: bfloat16 [4, 24576, 1024], P('dp', 'ctx')
The draws below stay inside these ranges and needn't reach their ends.
Inputs may be any that keep to these rules, and one draw needn't show every extreme that they name: For each sequence, dest_shard and dest_row together map its 24576 tokens one to one onto the 24576 packed positions. Among the tokens of one device (aligned blocks of 384), at most 12 have the same dest_shard, and in every draw some block has exactly 12 for some shard. `dest_row`: see dest_shard. `segments`: segment numbers never fall along a sequence; each segment holds 1 to 384 positions.
All inputs are finite; a program needn't handle non-finite values. No bound on the sum of `modality` on one device may be relied on, other than what follows from the above.
Results may differ from the reference program's by a relative error of at most 0.006.
Values may be sent and summed in bfloat16 or wider, within the bound.
A program may use at most 128 MiB of HBM per device.

```python
import math
import jax
import jax.numpy as jnp
import numpy as np
from jax import lax

D = 1024
HEADS = 16
FF = 2048
SEQ_DEV = 384
SEQ = 24576
BATCH = 4
CAP = 12
N_CTX = 64


def one_plan(seed_key):
    shards = SEQ // SEQ_DEV
    half_cap = CAP // 2
    key_a, key_b, key_c, key_d, key_e = jax.random.split(seed_key, 5)
    pairing = jax.random.permutation(key_a, shards)
    moved = jax.random.randint(key_b, (shards // 2,), 0, half_cap + 1).at[0].set(half_cap)
    loads = jnp.full((shards,), half_cap, jnp.int32).at[pairing[0::2]].add(moved).at[pairing[1::2]].add(-moved)
    offsets = jax.random.permutation(key_c, shards)
    sources = jnp.arange(shards, dtype=jnp.int32)
    targets = (sources[:, None] + offsets[None, :]) % shards
    source_grid = jnp.broadcast_to(sources[:, None], (shards, shards))
    counts = jnp.zeros((shards, shards), jnp.int32).at[source_grid, targets].add(jnp.broadcast_to(loads[None, :], (shards, shards)))
    bounds = jnp.cumsum(counts, axis=1)
    ranks = jnp.arange(SEQ_DEV, dtype=jnp.int32)
    sorted_dest = jnp.sum((bounds[:, None, :] <= ranks[None, :, None]).astype(jnp.int32), axis=2)
    shuffles = jax.vmap(lambda sub_key: jax.random.permutation(sub_key, SEQ_DEV))(jax.random.split(key_d, shards))
    plan_shard = jnp.take_along_axis(sorted_dest, shuffles, axis=1).reshape(-1)
    chosen = (plan_shard[:, None] == sources[None, :]).astype(jnp.int32)
    arrival = jnp.sum((jnp.cumsum(chosen, axis=0) - chosen) * chosen, axis=1)
    placements = jax.vmap(lambda sub_key: jax.random.permutation(sub_key, SEQ_DEV))(jax.random.split(key_e, shards))
    plan_row = placements[plan_shard, arrival]
    return (plan_shard.astype(jnp.int32), plan_row.astype(jnp.int32))


def packing_plan(key):
    plan_key = jax.random.fold_in(key, 17)
    return jax.vmap(one_plan)(jax.random.split(plan_key, BATCH))


def draw_dest_shard(key, part):
    return packing_plan(key)[0]


def draw_dest_row(key, part):
    return packing_plan(key)[1]


def draw_w_qkv(key, part):
    key_a = jax.random.fold_in(jax.random.fold_in(key, 29), 0)
    base = jax.random.normal(key_a, (D, 3 * D), jnp.float32) / jnp.sqrt(jnp.float32(D))
    return base.astype(jnp.bfloat16)


def plant(values, key, least, top_value):
    longest = values.shape.index(max(values.shape))
    spots = []
    for shift in (0, 1):
        where = [jax.random.randint(jax.random.fold_in(key, axis), (), 0, length) for axis, length in enumerate(values.shape)]
        where[longest] = (where[longest] + shift) % values.shape[longest]
        spots.append(tuple(where))
    return values.at[spots[0]].set(least).at[spots[1]].set(top_value)


def block_levels(key, extent, pieces, low, top_value):
    def one(dim, shards_of):
        draws = jax.random.uniform(jax.random.fold_in(jax.random.fold_in(key, 6), dim), (shards_of,), jnp.float32, low / len(pieces), top_value / len(pieces))
        return jnp.repeat(jnp.exp(draws), extent[dim] // shards_of).reshape((-1,) + (1,) * (len(extent) - dim - 1))

    loudness = one(*pieces[0])
    for cut in pieces[1:]:
        loudness = loudness * one(*cut)
    return loudness


def split_up(number_of, total, bound, skew):
    weights = [(1 << 20) // math.isqrt(rank ** skew) + 1 for rank in range(2, number_of + 1)]
    surplus, given = total - bound - (number_of - 1), [1] * (number_of - 1)
    while surplus > 0:
        free = [i for i in range(number_of - 1) if given[i] < bound]
        whole, remaining = sum([weights[i] for i in free]), surplus
        for i in free:
            more = min(bound - given[i], max(1, remaining * weights[i] // whole), surplus)
            given[i] = given[i] + more
            surplus = surplus - more
    return np.array([bound] + given)


def uneven_parts(own_key, number_of, total, reach, lean):
    if number_of == 2:
        one = jax.random.randint(own_key, (), max(1, total - reach), min(reach, total - 1) + 1)
        return jnp.stack([one, total - one])
    sizes = jnp.asarray(split_up(number_of, total, reach, lean), jnp.int32)
    couples = (number_of - 1) // 2
    donor, sink = sizes[1:1 + 2 * couples:2], sizes[2:2 + 2 * couples:2]
    slack = jnp.minimum(donor - 1, reach - sink)
    moved = jax.random.randint(jax.random.fold_in(own_key, 1), (couples,), 0, 1 << 20) % (slack + 1)
    sizes = sizes.at[1:1 + 2 * couples:2].set(donor - moved).at[2:2 + 2 * couples:2].set(sink + moved)
    return sizes[jax.random.permutation(jax.random.fold_in(own_key, 2), number_of)]


def centred(stream_key, extent, scale, bound, cuts=(), held_as=jnp.bfloat16):
    values = scale * jax.random.normal(stream_key, extent, jnp.float32)
    if cuts:
        values = values * block_levels(stream_key, extent, cuts, -0.22, 0.18)
    return jnp.clip(values, -bound, bound).astype(held_as)


def setup_inputs(seed: int = 0) -> dict:
    key_of = jax.random.split(jax.random.key(seed), 11)
    return {
        "tokens": centred(key_of[0], (BATCH, SEQ, D), 1.0, 6.0, ((0, 4), (1, 64))),
        "modality": plant((jax.random.randint(key_of[1], (BATCH, SEQ), 0, 3) < 1).astype(jnp.int32), jax.random.fold_in(key_of[1], 1), 0, 1),
        "type_embed": centred(key_of[2], (2, D), 1.0, 6.0),
        "dest_shard": draw_dest_shard(jax.random.fold_in(key_of[10], 71), 0),
        "dest_row": draw_dest_row(jax.random.fold_in(key_of[10], 71), 0),
        "segments": jax.vmap(lambda own: jnp.searchsorted(jnp.cumsum(uneven_parts(own, 2 * SEQ // SEQ_DEV, SEQ, SEQ_DEV, 0)), jnp.arange(SEQ), side="right"))(jax.random.split(key_of[5], BATCH)).reshape((BATCH, SEQ)).astype(jnp.int32),
        "w_qkv": draw_w_qkv(jax.random.fold_in(key_of[10], 71), 0),
        "w_out": centred(key_of[7], (D, D), D ** -0.5, 0.1875, ((0, 64), (1, 4))),
        "w_up": centred(key_of[8], (D, FF), D ** -0.5, 0.1875, ((0, 64), (1, 4))),
        "w_down": centred(key_of[9], (FF, D), FF ** -0.5, 0.125, ((0, 64), (1, 4))),
    }


norm_eps = 1e-06

def layer_norm(values):
    row_mean = lax.optimization_barrier(jnp.mean(values, axis=-1, keepdims=True))
    centered = values - row_mean
    spread = lax.optimization_barrier(jnp.mean(centered * centered, axis=-1, keepdims=True))
    return centered * lax.rsqrt(spread + norm_eps)

def attend(queries, key_pairs, query_seg, key_seg):
    seq_rows = queries.shape[0]
    key_span = key_pairs.shape[0]
    head_dim = D // HEADS
    query_heads = queries.reshape(seq_rows, HEADS, head_dim).astype(jnp.float32)
    key_heads = key_pairs[:, :D].reshape(key_span, HEADS, head_dim).astype(jnp.float32)
    value_heads = key_pairs[:, D:].reshape(key_span, HEADS, head_dim).astype(jnp.float32)
    allowed = query_seg[:, None] == key_seg[None, :]
    scores = jnp.einsum('qhd,khd->hqk', query_heads, key_heads) * head_dim ** (-0.5)
    scores = jnp.where(allowed[None], scores, -1e+30)
    row_max = lax.optimization_barrier(jnp.max(scores, axis=-1, keepdims=True))
    expd = jnp.exp(scores - row_max)
    attn_probs = (expd / lax.optimization_barrier(jnp.sum(expd, axis=-1, keepdims=True))).astype(jnp.bfloat16)
    head_mix = jnp.einsum('hqk,khd->qhd', attn_probs.astype(jnp.float32), value_heads)
    return head_mix.reshape(seq_rows, D).astype(jnp.bfloat16)

def encode(embedded, plan_shard, plan_row, seq_seg, w_qkv, w_out, w_up, w_down):
    place = plan_shard * SEQ_DEV + plan_row
    packed = jnp.zeros((SEQ, D), jnp.bfloat16).at[place].set(embedded)
    normed = layer_norm(packed.astype(jnp.float32)).astype(jnp.bfloat16)
    qkv_all = jnp.dot(normed, w_qkv, preferred_element_type=jnp.float32).astype(jnp.bfloat16)
    queries = qkv_all[:, :D]
    empty_rim = jnp.zeros((SEQ_DEV, 2 * D), jnp.bfloat16)
    key_pairs = jnp.concatenate([empty_rim, qkv_all[:, D:], empty_rim], axis=0)
    filler = jnp.full((SEQ_DEV,), -1, jnp.int32)
    padded_seg = jnp.concatenate([filler, seq_seg, filler])

    def one_block(block_index):
        offset = (block_index * SEQ_DEV).astype(jnp.int32)
        q_block = lax.dynamic_slice_in_dim(queries, offset, SEQ_DEV, 0)
        kv_block = lax.dynamic_slice_in_dim(key_pairs, offset, 3 * SEQ_DEV, 0)
        query_seg = lax.dynamic_slice_in_dim(seq_seg, offset, SEQ_DEV, 0)
        key_seg = lax.dynamic_slice_in_dim(padded_seg, offset, 3 * SEQ_DEV, 0)
        return attend(q_block, kv_block, query_seg, key_seg)
    attended = lax.map(one_block, jnp.arange(N_CTX, dtype=jnp.int32)).reshape(SEQ, D)
    middle = packed.astype(jnp.float32) + jnp.dot(attended, w_out, preferred_element_type=jnp.float32)
    normed_mid = layer_norm(middle).astype(jnp.bfloat16)
    hidden = jax.nn.gelu(jnp.dot(normed_mid, w_up, preferred_element_type=jnp.float32), approximate=True).astype(jnp.bfloat16)
    result = (middle + jnp.dot(hidden, w_down, preferred_element_type=jnp.float32)).astype(jnp.bfloat16)
    return result[place]

def reference(tokens, modality, type_embed, dest_shard, dest_row, segments, w_qkv, w_out, w_up, w_down):
    extra = jnp.where(modality[:, :, None] == 1, type_embed[1], type_embed[0]).astype(jnp.float32)
    embedded = (tokens.astype(jnp.float32) + extra).astype(jnp.bfloat16)
    outputs = []
    for seq_index in range(BATCH):
        outputs.append(encode(embedded[seq_index], dest_shard[seq_index], dest_row[seq_index], segments[seq_index], w_qkv, w_out, w_up, w_down))
    return jnp.stack(outputs)
```

```python
import jax
import jax.numpy as jnp
from jax import lax
from jax.experimental import pallas as pl
from jax.experimental.pallas import tpu as pltpu
from jax.sharding import Mesh
from jax.sharding import PartitionSpec as P

MESH = pl.DeviceIdType.MESH
CTX = ("ctx_0", "ctx_1", "ctx_2")
AXES = ("dp", *CTX)
NX, NZ, NY = 4, 8, 4
CHIPS = NX * NZ
ROWS = 384
WIDTH = 1024
HEADS = 16
FF = 2048
CAP = 12
BLOCK = 2 * CAP
SLOTS = CHIPS * BLOCK
BAND = 896
bf16, f32, i32 = jnp.bfloat16, jnp.float32, jnp.int32


def layer_norm(values):
    row_mean = jnp.mean(values, axis=-1, keepdims=True)
    centered = values - row_mean
    spread = jnp.mean(centered * centered, axis=-1, keepdims=True)
    return centered * lax.rsqrt(spread + 1e-06)


def dot(a, b):
    return jnp.dot(a, b, preferred_element_type=f32)


def iota(shape, dim):
    return lax.broadcasted_iota(i32, shape, dim)


def turned(row):
    return jnp.transpose(jnp.broadcast_to(row, (128, row.shape[1])))


def lanes(start, size):
    return pl.ds(pl.multiple_of(start, 128), size)


def kernel(
    tok, mod, temb, dsh, drow, seg, w_qkv, w_out, w_up, w_down, out,
    g_qkv, g_out, g_up, g_down, plan_s, plan_r, outbox, inbox, back, home,
    pick_back, pick_home, bias, packed, normed, q, k, v, att, mid, nmid, hidden, res,
    a_send, a_recv, ad_send, ad_recv, r_send, r_recv, rd_send, rd_recv, local_sem,
    z_send, z_recv, x_send, x_recv, y_send, y_recv, f_send, f_recv, d_send, d_recv,
    h_send, h_recv,
):
    y, x, z, c = [lax.axis_index(a) for a in AXES]
    chip = x * NZ + z
    own = 2 * chip + c
    partner = (y, x, z, 1 - c)
    shards = (w_qkv, w_out, w_up, w_down)
    full = (g_qkv, g_out, g_up, g_down)

    def place(j):
        tx = lax.rem(x + j // NZ, NX)
        tz = lax.rem(z + lax.rem(j, NZ), NZ)
        return tx, tz

    def remote(src, dst, send, recv, device):
        return pltpu.make_async_remote_copy(
            src_ref=src, dst_ref=dst, send_sem=send, recv_sem=recv,
            device_id=device, device_id_type=MESH,
        )

    right_chip = lax.rem(chip + 1, CHIPS)
    left_chip = lax.rem(chip + CHIPS - 1, CHIPS)
    far_chip = c * right_chip + (1 - c) * left_chip
    far = (y, far_chip // NZ, lax.rem(far_chip, NZ), 1 - c)

    barrier = pltpu.get_barrier_semaphore()

    def greet(j, _):
        tx, tz = place(j)
        pl.semaphore_signal(barrier, inc=1, device_id=(y, tx, tz, c), device_id_type=MESH)
        return 0

    lax.fori_loop(1, CHIPS, greet, 0)
    pl.semaphore_signal(barrier, inc=1, device_id=partner, device_id_type=MESH)
    pl.semaphore_signal(barrier, inc=1, device_id=far, device_id_type=MESH)
    for step in (1, NY - 1):
        pl.semaphore_signal(
            barrier, inc=1, device_id=(lax.rem(y + step, NY), x, z, c), device_id_type=MESH
        )

    def mine(w, col):
        size = shards[w].shape[1]
        return lanes(col * size, size)

    own_copies = [
        pltpu.make_async_copy(shards[w], full[w].at[chip, c, :, mine(w, y)], local_sem.at[w])
        for w in range(4)
    ]
    for cp in own_copies:
        cp.start()

    own_plan = dsh[:, lanes(own * ROWS, ROWS)]
    owner_ids = iota((64, ROWS), 0)
    chosen = owner_ids == own_plan
    before = (iota((ROWS, ROWS), 0) < iota((ROWS, ROWS), 1)).astype(bf16)
    ranks = dot(chosen.astype(f32).astype(bf16), before)
    earlier = jnp.sum(jnp.where(chosen, ranks, 0.0), axis=0, keepdims=True).astype(i32)
    slot = own_plan * CAP + earlier
    kinds = turned(mod[...])[:, :1]
    types = temb[...].astype(f32)
    extra = jnp.where(kinds == 1, types[1:2], types[0:1])
    att[...] = (tok[...].astype(f32) + extra).astype(bf16)

    pl.semaphore_wait(barrier, CHIPS - 1 + 4)

    def z_copy(w, j):
        return remote(
            shards[w], full[w].at[chip, c, :, mine(w, y)], z_send.at[w, j], z_recv.at[w, j],
            (y, x, lax.rem(z + j, NZ), c),
        )

    def x_copy(w, j):
        part = full[w].at[pl.ds(x * NZ, NZ), c, :, mine(w, y)]
        return remote(
            part, part, x_send.at[w, j], x_recv.at[w, j], (y, lax.rem(x + j, NX), z, c)
        )

    def y_copy(w, side):
        part = full[w].at[:, c, :, mine(w, y)]
        to = lax.rem(y + (1, NY - 1)[side], NY)
        return remote(part, part, y_send.at[w, side], y_recv.at[w, side], (to, x, z, c))

    def f_copy(w, side):
        held = lax.rem(y + (NY - 1, 1)[side], NY)
        part = full[w].at[pl.ds(side * (CHIPS // 2), CHIPS // 2), c, :, mine(w, held)]
        to = lax.rem(y + (1, NY - 1)[side], NY)
        return remote(part, part, f_send.at[w, side], f_recv.at[w, side], (to, x, z, c))

    def d_copy(w, step):
        part = full[w].at[:, c, :, mine(w, lax.rem(y + step, NY))]
        return remote(part, part, d_send.at[w, step], d_recv.at[w, step], partner)

    def each(count, act):
        def step(j, _):
            act(j)
            return 0

        lax.fori_loop(1, count, step, 0)

    def z_start(ws):
        for w in ws:
            each(NZ, lambda j: z_copy(w, j).start())

    def x_start(ws):
        for w in ws:
            own_copies[w].wait()
            each(NZ, lambda j: z_copy(w, j).wait())
            each(NX, lambda j: x_copy(w, j).start())

    def y_start(ws):
        for w in ws:
            each(NX, lambda j: x_copy(w, j).wait())
            y_copy(w, 0).start()
            y_copy(w, 1).start()
            d_copy(w, 0).start()

    def f_start(ws):
        for w in ws:
            y_copy(w, 0).wait()
            y_copy(w, 1).wait()
            f_copy(w, 0).start()
            f_copy(w, 1).start()
            d_copy(w, 1).start()
            d_copy(w, 3).start()

    def last_start(ws):
        for w in ws:
            f_copy(w, 0).wait()
            f_copy(w, 1).wait()
            d_copy(w, 2).start()

    def weights_done(w):
        for step in range(NY):
            d_copy(w, step).wait()

    first, rest = (0,), (1, 2, 3)
    z_start(first)

    embedded = att[...]

    def order(j):
        return (j // NZ) * NZ + lax.rem(3 * j, NZ)

    def a_copy(j):
        tx, tz = place(j)
        return remote(
            outbox.at[tx * NZ + tz], inbox.at[0, chip], a_send.at[j], a_recv.at[j], (y, tx, tz, c)
        )

    def pack(j, _):
        pick = (iota((SLOTS // NX, ROWS), 0) + j * (SLOTS // NX) == slot).astype(f32).astype(bf16)
        rows = dot(pick, embedded).astype(bf16)
        for i in range(NZ):
            outbox[j * NZ + i] = rows[i * BLOCK : (i + 1) * BLOCK]
        return 0

    lax.fori_loop(0, NX, pack, 0)
    own_block = pltpu.make_async_copy(outbox.at[chip], inbox.at[0, chip], local_sem.at[4])
    own_block.start()

    WAVE = 4

    def send_wave(n):
        def step(i, _):
            a_copy(order(i)).start()
            return 0

        lax.fori_loop(max(n * WAVE, 1), (n + 1) * WAVE, step, 0)

    def drain_wave(n):
        def step(i, _):
            a_copy(order(i)).wait_send()
            return 0

        lax.fori_loop(max(n * WAVE, 1), (n + 1) * WAVE, step, 0)

    send_wave(0)
    send_wave(1)
    x_start(first)

    def spread(j, _):
        part = lanes(j * ROWS, ROWS)
        plan_s[pl.ds(j, 1), :] = dsh[:, part]
        plan_r[pl.ds(j, 1), :] = drow[:, part]
        return 0

    drain_wave(0)
    send_wave(2)
    lax.fori_loop(0, 64, spread, 0)
    arriving = plan_s[...] == own
    arrival = dot(arriving.astype(f32).astype(bf16), before)
    rows_plus = plan_r[...].astype(f32) + 1.0
    drain_wave(1)
    send_wave(3)
    y_start(first)
    z_start(rest)
    slot_ids = iota((64, 128), 1)
    table = jnp.zeros((64, 128), f32)
    for n in range(CAP):
        hit = jnp.logical_and(arriving, arrival == float(n))
        value = jnp.sum(jnp.where(hit, rows_plus, 0.0), axis=1, keepdims=True)
        table = jnp.where(slot_ids == n, value, table)
    high = jnp.floor(table * (1.0 / 16.0))
    low = table - 16.0 * high
    lane = iota((128, SLOTS), 1)
    expand = (iota((128, SLOTS), 0) == lax.rem(lane, CAP)).astype(f32).astype(bf16)
    wide = 16.0 * dot(high.astype(bf16), expand) + dot(low.astype(bf16), expand)
    lane = iota((64, SLOTS), 1)
    source = iota((64, SLOTS), 0)

    def looked_up(wanted):
        return jnp.sum(jnp.where(source == wanted, wide, 0.0), axis=0, keepdims=True).astype(i32) - 1

    back_rows = looked_up(lane // CAP)
    other_rows = looked_up(2 * (lane // BLOCK) + (1 - c))
    lane_row = iota((1, SLOTS), 1)
    to_me = lax.rem(lane_row // CAP, 2) == c
    here_rows = jnp.where(to_me, back_rows, -1)
    other_rows = jnp.where(to_me, other_rows, -1)
    drain_wave(2)
    send_wave(4)
    f_start(first)
    x_start(rest)
    back_cols = turned(back_rows)
    for n in range(ROWS // 128):
        pick_back[:, 128 * n : 128 * (n + 1)] = (
            (back_cols == iota((SLOTS, 128), 1) + 128 * n).astype(f32).astype(bf16)
        )
    home_lane = (lax.rem(own_plan, 2) + c) % 2
    home_slot = home_lane * SLOTS + (own_plan // 2) * BLOCK + c * CAP + earlier
    home_cols = turned(home_slot)
    for n in range(2 * SLOTS // 128):
        pick_home[:, 128 * n : 128 * (n + 1)] = (
            (home_cols == iota((ROWS, 128), 1) + 128 * n).astype(f32).astype(bf16)
        )
    drain_wave(3)
    send_wave(5)

    q_seg = seg[:, lanes(own * ROWS, ROWS)]
    left_seg = seg[:, lanes(jnp.maximum(own - 1, 0) * ROWS, ROWS)]
    right_seg = seg[:, lanes(jnp.minimum(own + 1, 63) * ROWS, ROWS)]
    left_seg = jnp.where(own == 0, -1, left_seg)
    right_seg = jnp.where(own == 63, -1, right_seg)
    k_seg = jnp.concatenate([left_seg, q_seg, right_seg], axis=1)
    q_cols = turned(q_seg)
    for a in range(3):
        for n in range(BAND // 128):
            keys = k_seg[:, 128 * (a + n) : 128 * (a + n + 1)]
            same = q_cols[128 * a : 128 * (a + 1)] == keys
            bias[a, :, 128 * n : 128 * (n + 1)] = jnp.where(same, 0.0, -1e30)

    drain_wave(4)
    send_wave(6)
    last_start(first)
    drain_wave(5)
    send_wave(7)
    y_start(rest)
    drain_wave(6)
    drain_wave(7)

    def forward(src, send, recv, n):
        part = lax.rem(x + NX - n, NX)
        return remote(
            src.at[0, pl.ds(part * NZ, NZ)], src.at[1, pl.ds(part * NZ, NZ)],
            send.at[n], recv.at[n], partner,
        )

    own_block.wait()
    for n in range(NX):

        def arrive(j, _):
            a_copy(j).wait_recv()
            return 0

        lax.fori_loop(max(n * NZ, 1), (n + 1) * NZ, arrive, 0)
        forward(inbox, ad_send, ad_recv, n).start()
    for n in range(NX):
        forward(inbox, ad_send, ad_recv, n).wait()

    pick_here = (iota((ROWS, SLOTS), 0) == here_rows).astype(f32).astype(bf16)
    pick_other = (iota((ROWS, SLOTS), 0) == other_rows).astype(f32).astype(bf16)
    rows = dot(pick_here, inbox[0].reshape(SLOTS, WIDTH)) + dot(
        pick_other, inbox[1].reshape(SLOTS, WIDTH)
    )
    packed[...] = rows.astype(bf16)
    normed[1] = layer_norm(rows).astype(bf16)

    def h_copy(side):
        goes_right = c == 1 if side else c == 0
        slot = jnp.where(goes_right, 0, 2)
        return remote(
            normed.at[1], normed.at[slot], h_send.at[side], h_recv.at[side], (partner, far)[side]
        )

    h_copy(0).start()
    h_copy(1).start()

    weights_done(0)
    TILE = 256

    def columns(rows, weight, start, count, store):
        def step(j, _):
            part = lanes(start + j * TILE, TILE)
            w = weight[:, :, :, part]
            store(j, dot(rows, w.reshape(w.shape[0] * w.shape[1] * w.shape[2], TILE)))
            return 0

        lax.fori_loop(0, count // TILE, step, 0)

    def store_q(j, value):
        q[:, lanes(j * TILE, TILE)] = (value * 0.125).astype(bf16)

    def store_kv(block):
        at = pl.ds(block * ROWS, ROWS)

        def store_k(j, value):
            k[at, lanes(j * TILE, TILE)] = value.astype(bf16)

        def store_v(j, value):
            v[at, lanes(j * TILE, TILE)] = value.astype(bf16)

        return store_k, store_v

    own_rows = normed[1]
    columns(own_rows, g_qkv, 0, WIDTH, store_q)
    for block, side in ((1, None), (None, 0), (None, 1)):
        if side is not None:
            h_copy(side).wait()
        else:
            store_k, store_v = store_kv(1)
            columns(own_rows, g_qkv, WIDTH, WIDTH, store_k)
            columns(own_rows, g_qkv, 2 * WIDTH, WIDTH, store_v)
    for block in (0, 2):
        near_rows = normed[block]
        store_k, store_v = store_kv(block)
        columns(near_rows, g_qkv, WIDTH, WIDTH, store_k)
        columns(near_rows, g_qkv, 2 * WIDTH, WIDTH, store_v)
    f_start(rest)

    low_half = iota((128, 128), 1) < 64

    def attend(a):
        def step(h, _):
            part = lanes(h * 128, 128)
            rows = slice(128 * a, 128 * (a + 1))
            span = slice(128 * a, 128 * a + BAND)
            queries, keys, values = q[rows, part], k[span, part], v[span, part]
            mixed = []
            for half in (low_half, jnp.logical_not(low_half)):
                picked = jnp.where(half, queries.astype(f32), 0.0).astype(bf16)
                scores = lax.dot_general(
                    picked, keys, (((1,), (1,)), ((), ())), preferred_element_type=f32
                )
                scores = scores + bias[a]
                expd = jnp.exp(scores - jnp.max(scores, axis=1, keepdims=True))
                total = jnp.sum(expd, axis=1, keepdims=True)
                mixed.append(dot(expd.astype(bf16), values) / total)
            att[rows, part] = jnp.where(low_half, mixed[0], mixed[1]).astype(bf16)
            return 0

        lax.fori_loop(0, HEADS // 2, step, 0)

    attend(0)
    attend(1)
    last_start(rest)
    attend(2)

    weights_done(1)

    def store_mid(j, value):
        part = lanes(j * TILE, TILE)
        mid[:, part] = packed[:, part].astype(f32) + value

    columns(att[...], g_out, 0, WIDTH, store_mid)
    nmid[...] = layer_norm(mid[...]).astype(bf16)
    weights_done(2)

    def store_hidden(j, value):
        hidden[:, lanes(j * TILE, TILE)] = jax.nn.gelu(value, approximate=True).astype(bf16)

    columns(nmid[...], g_up, 0, FF, store_hidden)
    weights_done(3)

    def store_res(j, value):
        part = lanes(j * TILE, TILE)
        res[:, part] = (mid[:, part] + value).astype(bf16)

    columns(hidden[...], g_down, 0, WIDTH, store_res)

    result = res[...]

    def r_copy(j):
        tx, tz = place(j)
        return remote(
            back.at[tx * NZ + tz], home.at[0, chip], r_send.at[j], r_recv.at[j], (y, tx, tz, c)
        )

    def pack_back(j, _):
        at = pl.ds(pl.multiple_of(j * (SLOTS // NX), 16), SLOTS // NX)
        rows = dot(pick_back[at, :], result).astype(bf16)
        for i in range(NZ):
            back[j * NZ + i] = rows[i * BLOCK : (i + 1) * BLOCK]
        return 0

    lax.fori_loop(0, NX, pack_back, 0)
    home_block = pltpu.make_async_copy(back.at[chip], home.at[0, chip], local_sem.at[5])
    home_block.start()
    each(CHIPS, lambda i: r_copy(order(i)).start())
    home_block.wait()
    for n in range(NX):

        def arrive_home(j, _):
            r_copy(j).wait_recv()
            return 0

        lax.fori_loop(max(n * NZ, 1), (n + 1) * NZ, arrive_home, 0)
        forward(home, rd_send, rd_recv, n).start()
    for n in range(NX):
        forward(home, rd_send, rd_recv, n).wait()
    out[...] = (
        dot(pick_home[:, :SLOTS], home[0].reshape(SLOTS, WIDTH))
        + dot(pick_home[:, SLOTS:], home[1].reshape(SLOTS, WIDTH))
    ).astype(bf16)
    each(CHIPS, lambda i: r_copy(i).wait_send())


def local(tokens, modality, type_embed, dest_shard, dest_row, segments, w_qkv, w_out, w_up, w_down):
    vmem = pl.BlockSpec(memory_space=pltpu.VMEM)
    dma = pltpu.SemaphoreType.DMA
    V = pltpu.VMEM
    result = pl.pallas_call(
        kernel,
        out_shape=jax.ShapeDtypeStruct((ROWS, WIDTH), bf16),
        in_specs=[vmem] * 10,
        out_specs=vmem,
        scratch_shapes=[
            V((CHIPS, 2, 16, 3 * WIDTH), bf16),
            V((CHIPS, 2, 16, WIDTH), bf16),
            V((CHIPS, 2, 16, FF), bf16),
            V((CHIPS, 2, 32, WIDTH), bf16),
            V((64, ROWS), i32),
            V((64, ROWS), i32),
            V((CHIPS, BLOCK, WIDTH), bf16),
            V((2, CHIPS, BLOCK, WIDTH), bf16),
            V((CHIPS, BLOCK, WIDTH), bf16),
            V((2, CHIPS, BLOCK, WIDTH), bf16),
            V((SLOTS, ROWS), bf16),
            V((ROWS, 2 * SLOTS), bf16),
            V((3, 128, BAND), f32),
            V((ROWS, WIDTH), bf16),
            V((3, ROWS, WIDTH), bf16),
            V((ROWS, WIDTH), bf16),
            V((3 * ROWS, WIDTH), bf16),
            V((3 * ROWS, WIDTH), bf16),
            V((ROWS, WIDTH), bf16),
            V((ROWS, WIDTH), f32),
            V((ROWS, WIDTH), bf16),
            V((ROWS, FF), bf16),
            V((ROWS, WIDTH), bf16),
            dma((CHIPS,)), dma((CHIPS,)), dma((NX,)), dma((NX,)),
            dma((CHIPS,)), dma((CHIPS,)), dma((NX,)), dma((NX,)), dma((6,)),
            dma((4, NZ)), dma((4, NZ)), dma((4, NX)), dma((4, NX)),
            dma((4, 2)), dma((4, 2)), dma((4, 2)), dma((4, 2)), dma((4, NY)), dma((4, NY)),
            dma((2,)), dma((2,)),
        ],
        compiler_params=pltpu.CompilerParams(
            collective_id=0, has_side_effects=True, vmem_limit_bytes=63 * 1024 * 1024
        ),
        name="encoder",
    )(tokens[0], modality, type_embed, dest_shard, dest_row, segments, w_qkv, w_out, w_up, w_down)
    return result[None]


def solution(mesh):
    torus = Mesh(mesh.devices.reshape(NY, NX, NZ, 2), AXES)
    return jax.shard_map(
        local,
        mesh=torus,
        in_specs=(
            P("dp", CTX, None),
            P("dp", CTX),
            P(),
            P("dp", None),
            P("dp", None),
            P("dp", None),
            P(CTX, "dp"),
            P(CTX, "dp"),
            P(CTX, "dp"),
            P(CTX, "dp"),
        ),
        out_specs=P("dp", CTX, None),
        check_vma=False,
    )
```

```python
import jax
import jax.numpy as jnp
from jax import lax
from jax.experimental import pallas as pl
from jax.experimental.pallas import tpu as pltpu
from jax.sharding import Mesh
from jax.sharding import PartitionSpec as P

MESH = pl.DeviceIdType.MESH
CTX = ("ctx_0", "ctx_1", "ctx_2")
AXES = ("dp", *CTX)
NX, NZ, NY = 4, 8, 4
CHIPS = NX * NZ
ROWS = 384
WIDTH = 1024
HEADS = 16
FF = 2048
CAP = 12
BLOCK = 2 * CAP
SLOTS = CHIPS * BLOCK
BAND = 896
bf16, f32, i32 = jnp.bfloat16, jnp.float32, jnp.int32


def layer_norm(values):
    row_mean = jnp.mean(values, axis=-1, keepdims=True)
    centered = values - row_mean
    spread = jnp.mean(centered * centered, axis=-1, keepdims=True)
    return centered * lax.rsqrt(spread + 1e-06)


def dot(a, b):
    return jnp.dot(a, b, preferred_element_type=f32)


def iota(shape, dim):
    return lax.broadcasted_iota(i32, shape, dim)


def turned(row):
    return jnp.transpose(jnp.broadcast_to(row, (128, row.shape[1])))


def lanes(start, size):
    return pl.ds(pl.multiple_of(start, 128), size)


def kernel(
    tok, mod, temb, dsh, drow, seg, w_qkv, w_out, w_up, w_down, out,
    g_qkv, g_out, g_up, g_down, plan_s, plan_r, outbox, inbox, back, home,
    pick_back, pick_home, bias, packed, normed, q, k, v, att, mid, nmid, hidden, res,
    a_send, a_recv, ad_send, ad_recv, r_send, r_recv, rd_send, rd_recv,
    z_send, z_recv, q_recv, x_send, x_recv, y_send, y_recv, f_send, f_recv, d_send, d_recv,
    h_send, h_recv,
):
    y, x, z, c = [lax.axis_index(a) for a in AXES]
    chip = x * NZ + z
    own = 2 * chip + c
    partner = (y, x, z, 1 - c)
    shards = (w_qkv, w_out, w_up, w_down)
    full = (g_qkv, g_out, g_up, g_down)

    def place(j):
        tx = lax.rem(x + j // NZ, NX)
        tz = lax.rem(z + lax.rem(j, NZ), NZ)
        return tx, tz

    def remote(src, dst, send, recv, device):
        return pltpu.make_async_remote_copy(
            src_ref=src, dst_ref=dst, send_sem=send, recv_sem=recv,
            device_id=device, device_id_type=MESH,
        )

    def await_bytes(ref, sem):
        pltpu.make_async_copy(ref, ref, sem).wait()

    right_chip = lax.rem(chip + 1, CHIPS)
    left_chip = lax.rem(chip + CHIPS - 1, CHIPS)
    far_chip = c * right_chip + (1 - c) * left_chip
    far = (y, far_chip // NZ, lax.rem(far_chip, NZ), 1 - c)

    barrier = pltpu.get_barrier_semaphore()

    def greet(j, _):
        tx, tz = place(j)
        pl.semaphore_signal(barrier, inc=1, device_id=(y, tx, tz, c), device_id_type=MESH)
        return 0

    lax.fori_loop(1, CHIPS, greet, 0)
    pl.semaphore_signal(barrier, inc=1, device_id=partner, device_id_type=MESH)
    pl.semaphore_signal(barrier, inc=1, device_id=far, device_id_type=MESH)
    for step in range(1, NY):
        pl.semaphore_signal(
            barrier, inc=1, device_id=(lax.rem(y + step, NY), x, z, c), device_id_type=MESH
        )

    def mine(w, col):
        size = shards[w].shape[1]
        return lanes(col * size, size)

    own_copies = [
        pltpu.make_async_copy(shards[w], full[w].at[chip, c, :, mine(w, y)], z_recv.at[w])
        for w in range(4)
    ]
    for cp in own_copies:
        cp.start()

    own_plan = dsh[:, lanes(own * ROWS, ROWS)]
    owner_ids = iota((64, ROWS), 0)
    chosen = owner_ids == own_plan
    before = (iota((ROWS, ROWS), 0) < iota((ROWS, ROWS), 1)).astype(bf16)
    ranks = dot(chosen.astype(f32).astype(bf16), before)
    earlier = jnp.sum(jnp.where(chosen, ranks, 0.0), axis=0, keepdims=True).astype(i32)
    slot = own_plan * CAP + earlier
    kinds = turned(mod[...])[:, :1]
    types = temb[...].astype(f32)
    extra = jnp.where(kinds == 1, types[1:2], types[0:1])
    att[...] = (tok[...].astype(f32) + extra).astype(bf16)

    embedded = att[...]

    def pack(j, _):
        pick = (iota((SLOTS // NX, ROWS), 0) + j * (SLOTS // NX) == slot).astype(f32).astype(bf16)
        rows = dot(pick, embedded).astype(bf16)
        for i in range(NZ):
            outbox[j * NZ + i] = rows[i * BLOCK : (i + 1) * BLOCK]
        return 0

    lax.fori_loop(0, NX, pack, 0)

    pl.semaphore_wait(barrier, CHIPS - 1 + 5)

    def at_y(w):
        return w != 3

    def block(w, middle, last):
        xi, yi = (middle, last) if at_y(w) else (last, middle)
        return full[w].at[pl.ds(xi * NZ, NZ), c, :, mine(w, yi)]

    def spot(w):
        return (x, y) if at_y(w) else (y, x)

    def device(w, middle, last):
        return (last, middle, z, c) if at_y(w) else (middle, last, z, c)

    def around(i, step):
        return lax.rem(i + 4 + step, 4)

    def z_copy(w, j):
        return remote(
            shards[w], full[w].at[chip, c, :, mine(w, y)], z_send.at[w], z_recv.at[w],
            (y, x, lax.rem(z + j, NZ), c),
        )

    def ring_copy(w, step, side):
        way = (1, NZ - 1)[side]
        held = lax.rem(z + (step - 1) * (NZ - way), NZ)
        part = full[w].at[x * NZ + held, c, :, mine(w, y)]
        src = shards[w] if step == 1 else part
        to = (y, x, lax.rem(z + way, NZ), c)
        return remote(src, part, z_send.at[w], q_recv.at[w - 1, step - 1, side], to)

    def ring_sides(w, step):
        return (0, 1) if step < 4 else (0,) if w < 3 else (1,)

    def ring_wait(step):
        for w in rest:
            for side in ring_sides(w, step):
                ring_copy(w, step, side).wait_recv()

    def ring_start(step):
        if step > 1:
            ring_wait(step - 1)
        for w in rest:
            for side in ring_sides(w, step):
                ring_copy(w, step, side).start()

    def m_copy(w, j):
        m, n = spot(w)
        part = block(w, m, n)
        return remote(part, part, x_send.at[w], x_recv.at[w, j], device(w, lax.rem(m + j, 4), n))

    def n_copy(w, side):
        m, n = spot(w)
        step = (1, -1)[side]
        xi, yi = (around(m, -step), n) if at_y(w) else (n, around(m, -step))
        half = NZ // 2
        ref = full[w].at[pl.ds(xi * NZ + side * half, half), c, :, mine(w, yi)]
        to = device(w, around(m, step), n)
        return remote(ref, ref, x_send.at[w], x_recv.at[w, 2 * side], to)

    def l_copy(w, side, part):
        m, n = spot(w)
        ref = block(w, around(m, -part), n)
        to = device(w, m, around(n, (1, -1)[side]))
        return remote(ref, ref, y_send.at[w], y_recv.at[w, side, part], to)

    def f_copy(w, part):
        m, n = spot(w)
        step = 1 if part < 2 else -1
        ref = block(w, around(m, -part), around(n, -step))
        to = device(w, m, around(n, step))
        return remote(ref, ref, f_send.at[w], f_recv.at[w], to)

    def d_copy(w, step):
        at = around(spot(w)[1], step)
        if at_y(w):
            part = full[w].at[:, c, :, mine(w, at)]
        else:
            part = full[w].at[pl.ds(at * NZ, NZ), c]
        return remote(part, part, d_send.at[w], d_recv.at[w], partner)

    def each(count, act):
        def step(j, _):
            act(j)
            return 0

        lax.fori_loop(1, count, step, 0)

    def z_start(w):
        each(NZ, lambda j: z_copy(w, j).start())

    def l_part(w, part):
        l_copy(w, 0, part).start()
        l_copy(w, 1, part).start()

    def m_start(w):
        if w == 0:
            await_bytes(full[w].at[pl.ds(x * NZ, NZ), c, :, mine(w, y)], z_recv.at[w])
        else:
            own_copies[w].wait()
        await_bytes(full[w].at[pl.ds(0, NZ - 1), c, :, mine(w, y)], z_send.at[w])
        m_copy(w, 1).start()
        m_copy(w, 3).start()
        l_part(w, 0)

    def l_start(w):
        m_copy(w, 1).wait_recv()
        n_copy(w, 0).start()
        l_part(w, 1)
        m_copy(w, 3).wait_recv()
        n_copy(w, 1).start()
        l_part(w, 3)

    def l_finish(w):
        n_copy(w, 0).wait_recv()
        n_copy(w, 1).wait_recv()
        l_part(w, 2)
        d_copy(w, 0).start()

    def f_start(w):
        for part in (0, 1, 3, 2):
            l_copy(w, 0, part).wait_recv()
            l_copy(w, 1, part).wait_recv()
            f_copy(w, part).start()
        d_copy(w, 1).start()
        d_copy(w, 3).start()

    def last_start(w):
        quarter = full[w].at[:, c, :, mine(w, 0)]
        await_bytes(quarter, f_recv.at[w])
        d_copy(w, 2).start()

    def weights_done(w):
        await_bytes(full[w].at[:, 1 - c], d_recv.at[w])

    def weights_sent(w):
        part = mine(w, 0)
        await_bytes(full[w].at[pl.ds(0, 3 * NZ), c, :, part], x_send.at[w])
        await_bytes(full[w].at[:, :, :, part], y_send.at[w])
        await_bytes(full[w].at[:, c, :, part], f_send.at[w])
        await_bytes(full[w].at[:, c], d_send.at[w])

    rest = (1, 2, 3)
    z_start(0)
    ring_start(1)

    def order(j):
        return (j // NZ) * NZ + lax.rem(3 * j, NZ)

    def place_wave(j):
        return 2 * (j // NZ) + lax.rem(3 * j, NZ) // WAVE

    WAVE = 4

    def a_copy(j):
        tx, tz = place(j)
        return remote(
            outbox.at[tx * NZ + tz], inbox.at[0, chip], a_send.at[place_wave(j)], a_recv.at[j // NZ], (y, tx, tz, c)
        )

    own_block = pltpu.make_async_copy(outbox.at[chip], inbox.at[0, chip], a_recv.at[0])
    own_block.start()

    def send_wave(n):
        def step(i, _):
            a_copy(order(i)).start()
            return 0

        lax.fori_loop(max(n * WAVE, 1), (n + 1) * WAVE, step, 0)

    def drain_wave(n):
        await_bytes(inbox.at[1, pl.ds(0, WAVE if n else WAVE - 1)], a_send.at[n])

    send_wave(0)
    send_wave(1)
    m_start(0)
    ring_start(2)

    def spread(j, _):
        part = lanes(j * ROWS, ROWS)
        plan_s[pl.ds(j, 1), :] = dsh[:, part]
        plan_r[pl.ds(j, 1), :] = drow[:, part]
        return 0

    drain_wave(0)
    send_wave(2)
    lax.fori_loop(0, 64, spread, 0)
    arriving = plan_s[...] == own
    arrival = dot(arriving.astype(f32).astype(bf16), before)
    rows_plus = plan_r[...].astype(f32) + 1.0
    drain_wave(1)
    send_wave(3)
    l_start(0)
    ring_start(3)
    slot_ids = iota((64, 128), 1)
    table = jnp.zeros((64, 128), f32)
    for n in range(CAP):
        hit = jnp.logical_and(arriving, arrival == float(n))
        value = jnp.sum(jnp.where(hit, rows_plus, 0.0), axis=1, keepdims=True)
        table = jnp.where(slot_ids == n, value, table)
    high = jnp.floor(table * (1.0 / 16.0))
    low = table - 16.0 * high
    lane = iota((128, SLOTS), 1)
    expand = (iota((128, SLOTS), 0) == lax.rem(lane, CAP)).astype(f32).astype(bf16)
    wide = 16.0 * dot(high.astype(bf16), expand) + dot(low.astype(bf16), expand)
    lane = iota((64, SLOTS), 1)
    source = iota((64, SLOTS), 0)

    def looked_up(wanted):
        return jnp.sum(jnp.where(source == wanted, wide, 0.0), axis=0, keepdims=True).astype(i32) - 1

    back_rows = looked_up(lane // CAP)
    other_rows = looked_up(2 * (lane // BLOCK) + (1 - c))
    lane_row = iota((1, SLOTS), 1)
    to_me = lax.rem(lane_row // CAP, 2) == c
    here_rows = jnp.where(to_me, back_rows, -1)
    other_rows = jnp.where(to_me, other_rows, -1)
    drain_wave(2)
    send_wave(4)
    l_finish(0)
    ring_start(4)
    back_cols = turned(back_rows)
    for n in range(ROWS // 128):
        pick_back[:, 128 * n : 128 * (n + 1)] = (
            (back_cols == iota((SLOTS, 128), 1) + 128 * n).astype(f32).astype(bf16)
        )
    home_lane = (lax.rem(own_plan, 2) + c) % 2
    home_slot = home_lane * SLOTS + (own_plan // 2) * BLOCK + c * CAP + earlier
    home_cols = turned(home_slot)
    for n in range(2 * SLOTS // 128):
        pick_home[:, 128 * n : 128 * (n + 1)] = (
            (home_cols == iota((ROWS, 128), 1) + 128 * n).astype(f32).astype(bf16)
        )
    drain_wave(3)
    send_wave(5)
    send_wave(6)
    send_wave(7)

    q_seg = seg[:, lanes(own * ROWS, ROWS)]
    left_seg = seg[:, lanes(jnp.maximum(own - 1, 0) * ROWS, ROWS)]
    right_seg = seg[:, lanes(jnp.minimum(own + 1, 63) * ROWS, ROWS)]
    left_seg = jnp.where(own == 0, -1, left_seg)
    right_seg = jnp.where(own == 63, -1, right_seg)
    k_seg = jnp.concatenate([left_seg, q_seg, right_seg], axis=1)
    q_cols = turned(q_seg)
    for a in range(3):
        for n in range(BAND // 128):
            keys = k_seg[:, 128 * (a + n) : 128 * (a + n + 1)]
            same = q_cols[128 * a : 128 * (a + 1)] == keys
            bias[a, :, 128 * n : 128 * (n + 1)] = jnp.where(same, 0.0, -1e30)

    f_start(0)
    ring_wait(4)
    for w in rest:
        m_start(w)
    drain_wave(4)
    drain_wave(5)
    drain_wave(6)
    drain_wave(7)
    last_start(0)

    def x_blocks(n):
        return pl.ds(lax.rem(x + NX - n, NX) * NZ, NZ)

    for n in range(NX):
        span = x_blocks(n)
        await_bytes(inbox.at[0, span], a_recv.at[n])
        remote(inbox.at[0, span], inbox.at[1, span], ad_send, ad_recv, partner).start()
    for w in rest:
        l_start(w)
    await_bytes(inbox.at[0], ad_send)
    await_bytes(inbox.at[1], ad_recv)

    pick_here = (iota((ROWS, SLOTS), 0) == here_rows).astype(f32).astype(bf16)
    pick_other = (iota((ROWS, SLOTS), 0) == other_rows).astype(f32).astype(bf16)
    rows = dot(pick_here, inbox[0].reshape(SLOTS, WIDTH)) + dot(
        pick_other, inbox[1].reshape(SLOTS, WIDTH)
    )
    packed[...] = rows.astype(bf16)
    normed[1] = layer_norm(rows).astype(bf16)

    NEAR = ROWS // 3
    pieces = ((0, NEAR), (NEAR, ROWS))

    def far_rows(n, begins):
        lo, hi = pieces[n]
        start = jnp.where(begins, lo, ROWS - hi)
        return pl.ds(pl.multiple_of(start, 128), hi - lo)

    near_copy = remote(
        normed.at[1], normed.at[2 * c], h_send.at[0], h_recv.at[0], partner
    )

    def far_copy(n):
        rows = far_rows(n, c == 0)
        return remote(
            normed.at[1, rows], normed.at[2 * (1 - c), rows], h_send.at[1 + n], h_recv.at[1 + n], far
        )

    near_copy.start()
    far_copy(0).start()
    far_copy(1).start()

    weights_done(0)
    TILE = 256

    def columns(rows, weight, start, count, store):
        def step(j, _):
            part = lanes(start + j * TILE, TILE)
            w = weight[:, :, :, part]
            store(j, dot(rows, w.reshape(w.shape[0] * w.shape[1] * w.shape[2], TILE)))
            return 0

        lax.fori_loop(0, count // TILE, step, 0)

    def store_q(j, value):
        q[:, lanes(j * TILE, TILE)] = (value * 0.125).astype(bf16)

    def keys_values(rows, at):
        def store_k(j, value):
            k[at, lanes(j * TILE, TILE)] = value.astype(bf16)

        def store_v(j, value):
            v[at, lanes(j * TILE, TILE)] = value.astype(bf16)

        columns(rows, g_qkv, WIDTH, WIDTH, store_k)
        columns(rows, g_qkv, 2 * WIDTH, WIDTH, store_v)

    def rows_at(start, size):
        return pl.ds(pl.multiple_of(start, 128), size)

    def far_keys(n):
        far_copy(n).wait()
        rows = far_rows(n, c == 1)
        keys_values(normed[2 * c, rows], rows_at(2 * c * ROWS + rows.start, rows.size))

    own_rows = normed[1]
    columns(own_rows, g_qkv, 0, WIDTH, store_q)
    keys_values(own_rows, rows_at(ROWS, ROWS))
    near_copy.wait()
    near = 2 * (1 - c)
    keys_values(normed[near], rows_at(near * ROWS, ROWS))
    for w in rest:
        l_finish(w)

    low_half = iota((128, 128), 1) < 64

    def attend(n):
        a = jnp.where(c == 1, n, 2 - n)
        rows = rows_at(128 * a, 128)
        span = rows_at(128 * a, BAND)

        def step(h, _):
            part = lanes(h * 128, 128)
            queries = q[rows, part].astype(f32)
            keys, values = k[span, part], v[span, part]
            both = jnp.concatenate(
                [jnp.where(low_half, queries, 0.0), jnp.where(low_half, 0.0, queries)], axis=0
            ).astype(bf16)
            scores = lax.dot_general(
                both, keys, (((1,), (1,)), ((), ())), preferred_element_type=f32
            )
            shut = bias[a]
            scores = jnp.concatenate([scores[:128] + shut, scores[128:] + shut], axis=0)
            expd = jnp.exp(scores - jnp.max(scores, axis=1, keepdims=True))
            total = jnp.sum(expd, axis=1, keepdims=True)
            mixed = dot(expd.astype(bf16), values) / total
            att[rows, part] = jnp.where(low_half, mixed[:128], mixed[128:]).astype(bf16)
            return 0

        lax.fori_loop(0, HEADS // 2, step, 0)

    far_keys(0)
    attend(0)
    for w in rest:
        f_start(w)
    far_keys(1)
    attend(1)
    last_start(1)
    attend(2)
    last_start(2)
    last_start(3)

    weights_done(1)

    def store_mid(j, value):
        part = lanes(j * TILE, TILE)
        mid[:, part] = packed[:, part].astype(f32) + value

    columns(att[...], g_out, 0, WIDTH, store_mid)
    nmid[...] = layer_norm(mid[...]).astype(bf16)
    weights_done(2)

    def store_hidden(j, value):
        hidden[:, lanes(j * TILE, TILE)] = jax.nn.gelu(value, approximate=True).astype(bf16)

    columns(nmid[...], g_up, 0, FF, store_hidden)
    weights_done(3)

    HALF = WIDTH // 2

    def r_copy(half, j):
        tx, tz = place(j)
        part = pl.ds(half * HALF, HALF)
        return remote(
            back.at[tx * NZ + tz, :, part], home.at[0, chip, :, part],
            r_send.at[half], r_recv.at[half, j // NZ], (y, tx, tz, c),
        )

    for half in range(2):
        part = slice(half * HALF, (half + 1) * HALF)

        def store_res(j, value):
            at = lanes(half * HALF + j * TILE, TILE)
            res[:, at] = (mid[:, at] + value).astype(bf16)

        columns(hidden[...], g_down, half * HALF, HALF, store_res)
        result = res[:, part]

        def pack_back(j, _):
            at = pl.ds(pl.multiple_of(j * (SLOTS // NX), 16), SLOTS // NX)
            rows = dot(pick_back[at, :], result).astype(bf16)
            for i in range(NZ):
                back[j * NZ + i, :, part] = rows[i * BLOCK : (i + 1) * BLOCK]
            return 0

        lax.fori_loop(0, NX, pack_back, 0)
        pltpu.make_async_copy(
            back.at[chip, :, pl.ds(half * HALF, HALF)],
            home.at[0, chip, :, pl.ds(half * HALF, HALF)],
            r_recv.at[half, 0],
        ).start()
        each(CHIPS, lambda i: r_copy(half, order(i)).start())

    for half in range(2):
        part = slice(half * HALF, (half + 1) * HALF)
        cols = pl.ds(half * HALF, HALF)
        for n in range(NX):
            span = x_blocks(n)
            await_bytes(home.at[0, span, :, cols], r_recv.at[half, n])
            remote(
                home.at[0, span, :, cols], home.at[1, span, :, cols],
                rd_send.at[half], rd_recv.at[half], partner,
            ).start()
        await_bytes(home.at[1, :, :, cols], rd_recv.at[half])
        out[:, part] = (
            dot(pick_home[:, :SLOTS], home[0, :, :, part].reshape(SLOTS, HALF))
            + dot(pick_home[:, SLOTS:], home[1, :, :, part].reshape(SLOTS, HALF))
        ).astype(bf16)
    for half in range(2):
        cols = pl.ds(half * HALF, HALF)
        await_bytes(home.at[0, pl.ds(0, CHIPS - 1), :, cols], r_send.at[half])
        await_bytes(home.at[0, :, :, cols], rd_send.at[half])
    for w in range(4):
        weights_sent(w)


def local(tokens, modality, type_embed, dest_shard, dest_row, segments, w_qkv, w_out, w_up, w_down):
    vmem = pl.BlockSpec(memory_space=pltpu.VMEM)
    dma = pltpu.SemaphoreType.DMA
    V = pltpu.VMEM
    result = pl.pallas_call(
        kernel,
        out_shape=jax.ShapeDtypeStruct((ROWS, WIDTH), bf16),
        in_specs=[vmem] * 10,
        out_specs=vmem,
        scratch_shapes=[
            V((CHIPS, 2, 16, 3 * WIDTH), bf16),
            V((CHIPS, 2, 16, WIDTH), bf16),
            V((CHIPS, 2, 16, FF), bf16),
            V((CHIPS, 2, 32, WIDTH), bf16),
            V((64, ROWS), i32),
            V((64, ROWS), i32),
            V((CHIPS, BLOCK, WIDTH), bf16),
            V((2, CHIPS, BLOCK, WIDTH), bf16),
            V((CHIPS, BLOCK, WIDTH), bf16),
            V((2, CHIPS, BLOCK, WIDTH), bf16),
            V((SLOTS, ROWS), bf16),
            V((ROWS, 2 * SLOTS), bf16),
            V((3, 128, BAND), f32),
            V((ROWS, WIDTH), bf16),
            V((3, ROWS, WIDTH), bf16),
            V((ROWS, WIDTH), bf16),
            V((3 * ROWS, WIDTH), bf16),
            V((3 * ROWS, WIDTH), bf16),
            V((ROWS, WIDTH), bf16),
            V((ROWS, WIDTH), f32),
            V((ROWS, WIDTH), bf16),
            V((ROWS, FF), bf16),
            V((ROWS, WIDTH), bf16),
            dma((8,)), dma((NX,)), dma, dma,
            dma((2,)), dma((2, NX)), dma((2,)), dma((2,)),
            dma((4,)), dma((4,)), dma((3, 4, 2)), dma((4,)), dma((4, 4)),
            dma((4,)), dma((4, 2, 4)), dma((4,)), dma((4,)), dma((4,)), dma((4,)),
            dma((3,)), dma((3,)),
        ],
        compiler_params=pltpu.CompilerParams(
            collective_id=0, has_side_effects=True, vmem_limit_bytes=63 * 1024 * 1024
        ),
        name="encoder",
    )(tokens[0], modality, type_embed, dest_shard, dest_row, segments, w_qkv, w_out, w_up, w_down)
    return result[None]


def solution(mesh):
    torus = Mesh(mesh.devices.reshape(NY, NX, NZ, 2), AXES)
    return jax.shard_map(
        local,
        mesh=torus,
        in_specs=(
            P("dp", CTX, None),
            P("dp", CTX),
            P(),
            P("dp", None),
            P("dp", None),
            P("dp", None),
            P(CTX, "dp"),
            P(CTX, "dp"),
            P(CTX, "dp"),
            P(CTX, "dp"),
        ),
        out_specs=P("dp", CTX, None),
        check_vma=False,
    )
```

```python
import jax
import jax.numpy as jnp
from jax import lax
from jax.experimental import pallas as pl
from jax.experimental.pallas import tpu as pltpu
from jax.sharding import Mesh
from jax.sharding import PartitionSpec as P

MESH = pl.DeviceIdType.MESH
CTX = ("ctx_0", "ctx_1", "ctx_2")
AXES = ("dp", *CTX)
NX, NZ, NY = 4, 8, 4
CHIPS = NX * NZ
ROWS = 384
WIDTH = 1024
HEADS = 16
FF = 2048
CAP = 12
BLOCK = 2 * CAP
SLOTS = CHIPS * BLOCK
BAND = 896
bf16, f32, i32 = jnp.bfloat16, jnp.float32, jnp.int32


def layer_norm(values):
    row_mean = jnp.mean(values, axis=-1, keepdims=True)
    centered = values - row_mean
    spread = jnp.mean(centered * centered, axis=-1, keepdims=True)
    return centered * lax.rsqrt(spread + 1e-06)


def dot(a, b):
    return jnp.dot(a, b, preferred_element_type=f32)


def iota(shape, dim):
    return lax.broadcasted_iota(i32, shape, dim)


def turned(row):
    return jnp.transpose(jnp.broadcast_to(row, (128, row.shape[1])))


def lanes(start, size):
    return pl.ds(pl.multiple_of(start, 128), size)


def kernel(
    tok_in, mod_in, temb_in, dsh_in, drow_in, seg_in, w_qkv, w_out, w_up, w_down, out,
    tok, mod, temb, dsh, drow, seg, in_sem, own_sem,
    g_qkv, g_out, g_up, g_down, plan_s, plan_r, outbox, inbox, back, home,
    pick_back, pick_home, bias, packed, normed, q, k, v, att, mid, nmid, hidden, res,
    a_send, a_recv, ad_send, ad_recv, r_send, r_recv, rd_send, rd_recv,
    z_send, z_recv, q_recv, x_send, x_recv, y_send, y_recv, f_send, f_recv, d_send, d_recv,
    h_send, h_recv,
):
    y, x, z, c = [lax.axis_index(a) for a in AXES]
    chip = x * NZ + z
    own = 2 * chip + c
    partner = (y, x, z, 1 - c)
    shards = (w_qkv, w_out, w_up, w_down)
    full = (g_qkv, g_out, g_up, g_down)

    def place(j):
        tx = lax.rem(x + j // NZ, NX)
        tz = lax.rem(z + lax.rem(j, NZ), NZ)
        return tx, tz

    def remote(src, dst, send, recv, device):
        return pltpu.make_async_remote_copy(
            src_ref=src, dst_ref=dst, send_sem=send, recv_sem=recv,
            device_id=device, device_id_type=MESH,
        )

    def await_bytes(ref, sem):
        pltpu.make_async_copy(ref, ref, sem).wait()

    right_chip = lax.rem(chip + 1, CHIPS)
    left_chip = lax.rem(chip + CHIPS - 1, CHIPS)
    far_chip = c * right_chip + (1 - c) * left_chip
    far = (y, far_chip // NZ, lax.rem(far_chip, NZ), 1 - c)

    barrier = pltpu.get_barrier_semaphore()

    def greet(j, _):
        tx, tz = place(j)
        pl.semaphore_signal(barrier, inc=1, device_id=(y, tx, tz, c), device_id_type=MESH)
        return 0

    lax.fori_loop(1, CHIPS, greet, 0)
    pl.semaphore_signal(barrier, inc=1, device_id=partner, device_id_type=MESH)
    pl.semaphore_signal(barrier, inc=1, device_id=far, device_id_type=MESH)
    for step in range(1, NY):
        pl.semaphore_signal(
            barrier, inc=1, device_id=(lax.rem(y + step, NY), x, z, c), device_id_type=MESH
        )

    def mine(w, col):
        size = shards[w].shape[1]
        return lanes(col * size, size)

    own_copies = [
        pltpu.make_async_copy(shards[w], full[w].at[chip, c, :, mine(w, y)], own_sem.at[w])
        for w in range(4)
    ]
    inputs = [
        pltpu.make_async_copy(src, dst, in_sem.at[n])
        for n, (src, dst) in enumerate(
            ((dsh_in, dsh), (mod_in, mod), (temb_in, temb), (tok_in, tok), (drow_in, drow), (seg_in, seg))
        )
    ]
    for cp in inputs[:4] + own_copies + inputs[4:]:
        cp.start()
    for cp in inputs[:4]:
        cp.wait()

    own_plan = dsh[:, lanes(own * ROWS, ROWS)]
    owner_ids = iota((64, ROWS), 0)
    chosen = owner_ids == own_plan
    before = (iota((ROWS, ROWS), 0) < iota((ROWS, ROWS), 1)).astype(bf16)
    ranks = dot(chosen.astype(f32).astype(bf16), before)
    earlier = jnp.sum(jnp.where(chosen, ranks, 0.0), axis=0, keepdims=True).astype(i32)
    slot = own_plan * CAP + earlier
    kinds = turned(mod[...])[:, :1]
    types = temb[...].astype(f32)
    extra = jnp.where(kinds == 1, types[1:2], types[0:1])
    att[...] = (tok[...].astype(f32) + extra).astype(bf16)

    embedded = att[...]

    def pack(j, _):
        pick = (iota((SLOTS // NX, ROWS), 0) + j * (SLOTS // NX) == slot).astype(f32).astype(bf16)
        rows = dot(pick, embedded).astype(bf16)
        for i in range(NZ):
            outbox[j * NZ + i] = rows[i * BLOCK : (i + 1) * BLOCK]
        return 0

    lax.fori_loop(0, NX, pack, 0)

    for cp in own_copies + inputs[4:]:
        cp.wait()
    pl.semaphore_wait(barrier, CHIPS - 1 + 5)

    def at_y(w):
        return w != 3

    def block(w, middle, last):
        xi, yi = (middle, last) if at_y(w) else (last, middle)
        return full[w].at[pl.ds(xi * NZ, NZ), c, :, mine(w, yi)]

    def spot(w):
        return (x, y) if at_y(w) else (y, x)

    def device(w, middle, last):
        return (last, middle, z, c) if at_y(w) else (middle, last, z, c)

    def around(i, step):
        return lax.rem(i + 4 + step, 4)

    def z_copy(w, j):
        part = full[w].at[chip, c, :, mine(w, y)]
        return remote(part, part, z_send.at[w], z_recv.at[w], (y, x, lax.rem(z + j, NZ), c))

    def ring_copy(w, step, side):
        way = (1, NZ - 1)[side]
        held = lax.rem(z + (step - 1) * (NZ - way), NZ)
        part = full[w].at[x * NZ + held, c, :, mine(w, y)]
        to = (y, x, lax.rem(z + way, NZ), c)
        return remote(part, part, z_send.at[w], q_recv.at[w - 1, step - 1, side], to)

    def ring_sides(w, step):
        return (0, 1) if step < 4 else (0,) if w < 3 else (1,)

    def ring_wait(step):
        for w in rest:
            for side in ring_sides(w, step):
                ring_copy(w, step, side).wait_recv()

    def ring_start(step):
        if step > 1:
            ring_wait(step - 1)
        for w in rest:
            for side in ring_sides(w, step):
                ring_copy(w, step, side).start()

    def m_copy(w, j):
        m, n = spot(w)
        part = block(w, m, n)
        return remote(part, part, x_send.at[w], x_recv.at[w, j], device(w, lax.rem(m + j, 4), n))

    def n_copy(w, side):
        m, n = spot(w)
        step = (1, -1)[side]
        xi, yi = (around(m, -step), n) if at_y(w) else (n, around(m, -step))
        half = NZ // 2
        ref = full[w].at[pl.ds(xi * NZ + side * half, half), c, :, mine(w, yi)]
        to = device(w, around(m, step), n)
        return remote(ref, ref, x_send.at[w], x_recv.at[w, 2 * side], to)

    def l_copy(w, side, part):
        m, n = spot(w)
        ref = block(w, around(m, -part), n)
        to = device(w, m, around(n, (1, -1)[side]))
        return remote(ref, ref, y_send.at[w], y_recv.at[w, side, part], to)

    def f_copy(w, part):
        m, n = spot(w)
        step = 1 if part < 2 else -1
        ref = block(w, around(m, -part), around(n, -step))
        to = device(w, m, around(n, step))
        return remote(ref, ref, f_send.at[w], f_recv.at[w], to)

    def d_copy(w, step):
        at = around(spot(w)[1], step)
        if at_y(w):
            part = full[w].at[:, c, :, mine(w, at)]
        else:
            part = full[w].at[pl.ds(at * NZ, NZ), c]
        return remote(part, part, d_send.at[w], d_recv.at[w], partner)

    def each(count, act):
        def step(j, _):
            act(j)
            return 0

        lax.fori_loop(1, count, step, 0)

    def z_start(w):
        each(NZ, lambda j: z_copy(w, j).start())

    def l_part(w, part):
        l_copy(w, 0, part).start()
        l_copy(w, 1, part).start()

    def m_start(*ws):
        for w in ws:
            seven = full[w].at[pl.ds(0, NZ - 1), c, :, mine(w, y)]
            if w == 0:
                await_bytes(seven, z_recv.at[w])
            await_bytes(seven, z_send.at[w])
            m_copy(w, 1).start()
            m_copy(w, 3).start()
        for w in ws:
            l_part(w, 0)

    def n_start(*ws):
        for w in ws:
            m_copy(w, 1).wait_recv()
            n_copy(w, 0).start()
            m_copy(w, 3).wait_recv()
            n_copy(w, 1).start()

    def l_start(*ws):
        for w in ws:
            l_part(w, 1)
            l_part(w, 3)

    def l_finish(*ws):
        for w in ws:
            n_copy(w, 0).wait_recv()
            n_copy(w, 1).wait_recv()
            l_part(w, 2)
            d_copy(w, 0).start()

    def f_part(w, *parts):
        for part in parts:
            l_copy(w, 0, part).wait_recv()
            l_copy(w, 1, part).wait_recv()
            f_copy(w, part).start()

    def f_finish(w, *parts):
        f_part(w, *parts)
        d_copy(w, 1).start()
        d_copy(w, 3).start()

    def last_start(w):
        quarter = full[w].at[:, c, :, mine(w, 0)]
        await_bytes(quarter, f_recv.at[w])
        d_copy(w, 2).start()

    def weights_done(w):
        await_bytes(full[w].at[:, 1 - c], d_recv.at[w])

    def weights_sent(w):
        part = mine(w, 0)
        await_bytes(full[w].at[pl.ds(0, 3 * NZ), c, :, part], x_send.at[w])
        await_bytes(full[w].at[:, :, :, part], y_send.at[w])
        await_bytes(full[w].at[:, c, :, part], f_send.at[w])
        await_bytes(full[w].at[:, c], d_send.at[w])

    rest = (1, 2, 3)
    z_start(0)
    ring_start(1)

    def order(j):
        return (j // NZ) * NZ + lax.rem(3 * j, NZ)

    def place_wave(j):
        return 2 * (j // NZ) + lax.rem(3 * j, NZ) // WAVE

    WAVE = 4

    def a_copy(j):
        tx, tz = place(j)
        return remote(
            outbox.at[tx * NZ + tz], inbox.at[0, chip], a_send.at[place_wave(j)], a_recv.at[j // NZ], (y, tx, tz, c)
        )

    own_block = pltpu.make_async_copy(outbox.at[chip], inbox.at[0, chip], a_recv.at[0])
    own_block.start()

    def send_wave(n):
        def step(i, _):
            a_copy(order(i)).start()
            return 0

        lax.fori_loop(max(n * WAVE, 1), (n + 1) * WAVE, step, 0)

    def drain_wave(n):
        await_bytes(inbox.at[1, pl.ds(0, WAVE if n else WAVE - 1)], a_send.at[n])

    send_wave(0)
    send_wave(1)
    m_start(0)
    ring_start(2)

    def spread(j, _):
        part = lanes(j * ROWS, ROWS)
        plan_s[pl.ds(j, 1), :] = dsh[:, part]
        plan_r[pl.ds(j, 1), :] = drow[:, part]
        return 0

    drain_wave(0)
    send_wave(2)
    lax.fori_loop(0, 64, spread, 0)
    arriving = plan_s[...] == own
    arrival = dot(arriving.astype(f32).astype(bf16), before)
    rows_plus = plan_r[...].astype(f32) + 1.0
    drain_wave(1)
    send_wave(3)
    n_start(0)
    l_start(0)
    ring_start(3)
    slot_ids = iota((64, 128), 1)
    table = jnp.zeros((64, 128), f32)
    for n in range(CAP):
        hit = jnp.logical_and(arriving, arrival == float(n))
        value = jnp.sum(jnp.where(hit, rows_plus, 0.0), axis=1, keepdims=True)
        table = jnp.where(slot_ids == n, value, table)
    high = jnp.floor(table * (1.0 / 16.0))
    low = table - 16.0 * high
    lane = iota((128, SLOTS), 1)
    expand = (iota((128, SLOTS), 0) == lax.rem(lane, CAP)).astype(f32).astype(bf16)
    wide = 16.0 * dot(high.astype(bf16), expand) + dot(low.astype(bf16), expand)
    lane = iota((64, SLOTS), 1)
    source = iota((64, SLOTS), 0)

    def looked_up(wanted):
        return jnp.sum(jnp.where(source == wanted, wide, 0.0), axis=0, keepdims=True).astype(i32) - 1

    back_rows = looked_up(lane // CAP)
    other_rows = looked_up(2 * (lane // BLOCK) + (1 - c))
    lane_row = iota((1, SLOTS), 1)
    to_me = lax.rem(lane_row // CAP, 2) == c
    here_rows = jnp.where(to_me, back_rows, -1)
    other_rows = jnp.where(to_me, other_rows, -1)
    drain_wave(2)
    send_wave(4)
    f_part(0, 0)
    l_finish(0)
    f_part(0, 1)
    ring_start(4)
    back_cols = turned(back_rows)
    for n in range(ROWS // 128):
        pick_back[:, 128 * n : 128 * (n + 1)] = (
            (back_cols == iota((SLOTS, 128), 1) + 128 * n).astype(f32).astype(bf16)
        )
    home_lane = (lax.rem(own_plan, 2) + c) % 2
    home_slot = home_lane * SLOTS + (own_plan // 2) * BLOCK + c * CAP + earlier
    home_cols = turned(home_slot)
    for n in range(2 * SLOTS // 128):
        pick_home[:, 128 * n : 128 * (n + 1)] = (
            (home_cols == iota((ROWS, 128), 1) + 128 * n).astype(f32).astype(bf16)
        )
    drain_wave(3)
    send_wave(5)
    send_wave(6)
    send_wave(7)

    q_seg = seg[:, lanes(own * ROWS, ROWS)]
    left_seg = seg[:, lanes(jnp.maximum(own - 1, 0) * ROWS, ROWS)]
    right_seg = seg[:, lanes(jnp.minimum(own + 1, 63) * ROWS, ROWS)]
    left_seg = jnp.where(own == 0, -1, left_seg)
    right_seg = jnp.where(own == 63, -1, right_seg)
    k_seg = jnp.concatenate([left_seg, q_seg, right_seg], axis=1)
    q_cols = turned(q_seg)
    for a in range(3):
        for n in range(BAND // 128):
            keys = k_seg[:, 128 * (a + n) : 128 * (a + n + 1)]
            same = q_cols[128 * a : 128 * (a + 1)] == keys
            bias[a, :, 128 * n : 128 * (n + 1)] = jnp.where(same, 0.0, -1e30)

    f_finish(0, 3, 2)
    ring_wait(4)
    m_start(3, 1, 2)
    drain_wave(4)
    drain_wave(5)
    drain_wave(6)
    drain_wave(7)
    last_start(0)

    def x_blocks(n):
        return pl.ds(lax.rem(x + NX - n, NX) * NZ, NZ)

    for n in range(NX):
        span = x_blocks(n)
        await_bytes(inbox.at[0, span], a_recv.at[n])
        remote(inbox.at[0, span], inbox.at[1, span], ad_send, ad_recv, partner).start()
    await_bytes(inbox.at[0], ad_send)
    await_bytes(inbox.at[1], ad_recv)

    pick_here = (iota((ROWS, SLOTS), 0) == here_rows).astype(f32).astype(bf16)
    pick_other = (iota((ROWS, SLOTS), 0) == other_rows).astype(f32).astype(bf16)
    rows = dot(pick_here, inbox[0].reshape(SLOTS, WIDTH)) + dot(
        pick_other, inbox[1].reshape(SLOTS, WIDTH)
    )
    packed[...] = rows.astype(bf16)
    normed[1] = layer_norm(rows).astype(bf16)

    NEAR = ROWS // 3
    pieces = ((0, NEAR), (NEAR, ROWS))

    def far_rows(n, begins):
        lo, hi = pieces[n]
        start = jnp.where(begins, lo, ROWS - hi)
        return pl.ds(pl.multiple_of(start, 128), hi - lo)

    near_copy = remote(
        normed.at[1], normed.at[2 * c], h_send.at[0], h_recv.at[0], partner
    )

    def far_copy(n):
        rows = far_rows(n, c == 0)
        return remote(
            normed.at[1, rows], normed.at[2 * (1 - c), rows], h_send.at[1 + n], h_recv.at[1 + n], far
        )

    near_copy.start()
    n_start(3, 1, 2)
    far_copy(0).start()
    l_start(3, 1, 2)

    weights_done(0)
    TILE = 512

    def columns(rows, weight, start, count, store):
        def step(j, _):
            part = lanes(start + j * TILE, TILE)
            w = weight[:, :, :, part]
            store(j, dot(rows, w.reshape(w.shape[0] * w.shape[1] * w.shape[2], TILE)))
            return 0

        lax.fori_loop(0, count // TILE, step, 0)

    def store_q(j, value):
        q[:, lanes(j * TILE, TILE)] = (value * 0.125).astype(bf16)

    def keys_values(rows, at):
        def store_k(j, value):
            k[at, lanes(j * TILE, TILE)] = value.astype(bf16)

        def store_v(j, value):
            v[at, lanes(j * TILE, TILE)] = value.astype(bf16)

        columns(rows, g_qkv, WIDTH, WIDTH, store_k)
        columns(rows, g_qkv, 2 * WIDTH, WIDTH, store_v)

    def rows_at(start, size):
        return pl.ds(pl.multiple_of(start, 128), size)

    def far_keys(n):
        far_copy(n).wait()
        rows = far_rows(n, c == 1)
        keys_values(normed[2 * c, rows], rows_at(2 * c * ROWS + rows.start, rows.size))

    own_rows = normed[1]
    columns(own_rows, g_qkv, 0, WIDTH, store_q)
    keys_values(own_rows, rows_at(ROWS, ROWS))
    near_copy.wait()
    near = 2 * (1 - c)
    keys_values(normed[near], rows_at(near * ROWS, ROWS))
    l_finish(3, 1, 2)
    far_copy(1).start()

    low_half = iota((128, 128), 1) < 64

    def attend(n, heads=(0, HEADS // 2)):
        a = jnp.where(c == 1, n, 2 - n)
        rows = rows_at(128 * a, 128)
        span = rows_at(128 * a, BAND)

        def step(h, _):
            part = lanes(h * 128, 128)
            queries = q[rows, part].astype(f32)
            keys, values = k[span, part], v[span, part]
            both = jnp.concatenate(
                [jnp.where(low_half, queries, 0.0), jnp.where(low_half, 0.0, queries)], axis=0
            ).astype(bf16)
            scores = lax.dot_general(
                both, keys, (((1,), (1,)), ((), ())), preferred_element_type=f32
            )
            shut = bias[a]
            scores = jnp.concatenate([scores[:128] + shut, scores[128:] + shut], axis=0)
            expd = jnp.exp(scores - jnp.max(scores, axis=1, keepdims=True))
            total = jnp.sum(expd, axis=1, keepdims=True)
            mixed = dot(expd.astype(bf16), values) / total
            att[rows, part] = jnp.where(low_half, mixed[:128], mixed[128:]).astype(bf16)
            return 0

        lax.fori_loop(*heads, step, 0, unroll=4)

    far_keys(0)
    attend(0)
    for w in (1, 2):
        f_part(w, 0, 1, 3)
    far_keys(1)
    for w in (1, 2):
        f_finish(w, 2)
    attend(1, (0, HEADS // 4))
    f_finish(3, 0, 1, 3, 2)
    attend(1, (HEADS // 4, HEADS // 2))
    last_start(1)
    attend(2)
    last_start(2)
    last_start(3)

    weights_done(1)

    def store_mid(j, value):
        part = lanes(j * TILE, TILE)
        mid[:, part] = packed[:, part].astype(f32) + value

    columns(att[...], g_out, 0, WIDTH, store_mid)
    nmid[...] = layer_norm(mid[...]).astype(bf16)
    weights_done(2)

    def store_hidden(j, value):
        hidden[:, lanes(j * TILE, TILE)] = jax.nn.gelu(value, approximate=True).astype(bf16)

    columns(nmid[...], g_up, 0, FF, store_hidden)
    weights_done(3)

    HALF = WIDTH // 2

    def r_copy(half, j):
        tx, tz = place(j)
        part = pl.ds(half * HALF, HALF)
        return remote(
            back.at[tx * NZ + tz, :, part], home.at[0, chip, :, part],
            r_send.at[half], r_recv.at[half, j // NZ], (y, tx, tz, c),
        )

    for half in range(2):
        part = slice(half * HALF, (half + 1) * HALF)

        def store_res(j, value):
            at = lanes(half * HALF + j * TILE, TILE)
            res[:, at] = (mid[:, at] + value).astype(bf16)

        columns(hidden[...], g_down, half * HALF, HALF, store_res)
        result = res[:, part]

        def pack_back(j, _):
            at = pl.ds(pl.multiple_of(j * (SLOTS // NX), 16), SLOTS // NX)
            rows = dot(pick_back[at, :], result).astype(bf16)
            for i in range(NZ):
                back[j * NZ + i, :, part] = rows[i * BLOCK : (i + 1) * BLOCK]
            return 0

        lax.fori_loop(0, NX, pack_back, 0)
        pltpu.make_async_copy(
            back.at[chip, :, pl.ds(half * HALF, HALF)],
            home.at[0, chip, :, pl.ds(half * HALF, HALF)],
            r_recv.at[half, 0],
        ).start()
        each(CHIPS, lambda i: r_copy(half, order(i)).start())

    out_copies = []
    for half in range(2):
        part = slice(half * HALF, (half + 1) * HALF)
        cols = pl.ds(half * HALF, HALF)
        for n in range(NX):
            span = x_blocks(n)
            await_bytes(home.at[0, span, :, cols], r_recv.at[half, n])
            remote(
                home.at[0, span, :, cols], home.at[1, span, :, cols],
                rd_send.at[half], rd_recv.at[half], partner,
            ).start()
        await_bytes(home.at[1, :, :, cols], rd_recv.at[half])
        res[:, part] = (
            dot(pick_home[:, :SLOTS], home[0, :, :, part].reshape(SLOTS, HALF))
            + dot(pick_home[:, SLOTS:], home[1, :, :, part].reshape(SLOTS, HALF))
        ).astype(bf16)
        cp = pltpu.make_async_copy(res.at[:, part], out.at[:, part], own_sem.at[half])
        cp.start()
        out_copies.append(cp)
    for half in range(2):
        cols = pl.ds(half * HALF, HALF)
        await_bytes(home.at[0, pl.ds(0, CHIPS - 1), :, cols], r_send.at[half])
        await_bytes(home.at[0, :, :, cols], rd_send.at[half])
    for w in range(4):
        weights_sent(w)
    for cp in out_copies:
        cp.wait()


def local(tokens, modality, type_embed, dest_shard, dest_row, segments, w_qkv, w_out, w_up, w_down):
    dma = pltpu.SemaphoreType.DMA
    V = pltpu.VMEM
    result = pl.pallas_call(
        kernel,
        out_shape=jax.ShapeDtypeStruct((ROWS, WIDTH), bf16),
        in_specs=[pl.BlockSpec(memory_space=pltpu.HBM)] * 10,
        out_specs=pl.BlockSpec(memory_space=pltpu.HBM),
        scratch_shapes=[
            V((ROWS, WIDTH), bf16), V((1, ROWS), i32), V((2, WIDTH), bf16),
            V((1, 64 * ROWS), i32), V((1, 64 * ROWS), i32), V((1, 64 * ROWS), i32),
            dma((6,)), dma((4,)),
            V((CHIPS, 2, 16, 3 * WIDTH), bf16),
            V((CHIPS, 2, 16, WIDTH), bf16),
            V((CHIPS, 2, 16, FF), bf16),
            V((CHIPS, 2, 32, WIDTH), bf16),
            V((64, ROWS), i32),
            V((64, ROWS), i32),
            V((CHIPS, BLOCK, WIDTH), bf16),
            V((2, CHIPS, BLOCK, WIDTH), bf16),
            V((CHIPS, BLOCK, WIDTH), bf16),
            V((2, CHIPS, BLOCK, WIDTH), bf16),
            V((SLOTS, ROWS), bf16),
            V((ROWS, 2 * SLOTS), bf16),
            V((3, 128, BAND), f32),
            V((ROWS, WIDTH), bf16),
            V((3, ROWS, WIDTH), bf16),
            V((ROWS, WIDTH), bf16),
            V((3 * ROWS, WIDTH), bf16),
            V((3 * ROWS, WIDTH), bf16),
            V((ROWS, WIDTH), bf16),
            V((ROWS, WIDTH), f32),
            V((ROWS, WIDTH), bf16),
            V((ROWS, FF), bf16),
            V((ROWS, WIDTH), bf16),
            dma((8,)), dma((NX,)), dma, dma,
            dma((2,)), dma((2, NX)), dma((2,)), dma((2,)),
            dma((4,)), dma((4,)), dma((3, 4, 2)), dma((4,)), dma((4, 4)),
            dma((4,)), dma((4, 2, 4)), dma((4,)), dma((4,)), dma((4,)), dma((4,)),
            dma((3,)), dma((3,)),
        ],
        compiler_params=pltpu.CompilerParams(
            collective_id=0, has_side_effects=True, vmem_limit_bytes=58 * 1024 * 1024
        ),
        name="encoder",
    )(tokens[0], modality, type_embed, dest_shard, dest_row, segments, w_qkv, w_out, w_up, w_down)
    return result[None]


def solution(mesh):
    torus = Mesh(mesh.devices.reshape(NY, NX, NZ, 2), AXES)
    return jax.shard_map(
        local,
        mesh=torus,
        in_specs=(
            P("dp", CTX, None),
            P("dp", CTX),
            P(),
            P("dp", None),
            P("dp", None),
            P("dp", None),
            P(CTX, "dp"),
            P(CTX, "dp"),
            P(CTX, "dp"),
            P(CTX, "dp"),
        ),
        out_specs=P("dp", CTX, None),
        check_vma=False,
    )
```
